32 devices in a mesh: lon: 8 (over z, x), lat: 4 (over y, core).
Axes of the slice: x: 2, y: 2, z: 4, core: 2. Of those that a mesh axis runs over, the one named last changes fastest.
Arguments:
- state: float32 [2048, 64, 1024], P('lon', None, 'lat'), may hold values from -6 to 6
Outputs:
- spectrum: float32 [2, 1024, 64, 1024], P(None, 'lon', None, 'lat')
The draws below stay inside these ranges and needn't reach their ends.
All inputs are finite; a program needn't handle non-finite values.
Results may differ from the reference program's by a relative error of at most 0.00011.
Values sent between devices are 32-bit elements; how exact they have to be, the bound alone decides.
A program may use at most 128 MiB of HBM per device.

```python
import math
import jax
import jax.numpy as jnp

NLON = 2048
FIELDS = 64
NLAT = 1024
MODES = 1024


def steps_of(rng, shape, pieces, least, top_value):
    loudness = 1.0
    for dim, blocks in pieces:
        draws = jax.random.uniform(jax.random.fold_in(jax.random.fold_in(rng, 6), dim), (blocks,), jnp.float32, least / len(pieces), top_value / len(pieces))
        loudness = loudness * jnp.repeat(jnp.exp(draws), shape[dim] // blocks).reshape((-1,) + (1,) * (len(shape) - 1 - dim))
    return loudness


def noise(rng, dims, deviation, limit, shards=(), kind=jnp.bfloat16):
    array = jax.random.normal(rng, dims, jnp.float32) * deviation
    if len(shards) > 0:
        array = steps_of(rng, dims, shards, -0.22, 0.18) * array
    return jnp.clip(array, min=-limit, max=limit).astype(kind)


def setup_inputs(seed: int = 0) -> dict:
    arg_keys = jax.random.split(jax.random.key(seed), 2)
    return {
        "state": noise(arg_keys[0], (NLON, FIELDS, NLAT), 1.0, 6.0, ((0, 8), (2, 4)), jnp.float32),
    }


def reference(state):
    spectrum = jnp.fft.rfft(state, axis=0)[:MODES] * (1.0 / math.sqrt(NLON))
    return jnp.stack([jnp.real(spectrum), jnp.imag(spectrum)]).astype(jnp.float32)
```

```python
import functools
import math

import jax
import jax.numpy as jnp
import numpy as np
from jax import lax
from jax.experimental import pallas as pl
from jax.experimental.pallas import tpu as pltpu
from jax.sharding import PartitionSpec as P

RADIX = 8
LANES = 128
SUBLANES = 8
TILE = 16


def phase_angle(first_index, second_index, period):
    product = first_index * second_index % period
    return product.astype(jnp.float32) * (2.0 * math.pi / period)


def dense_spectrum(gathered, factor):
    lon_count = gathered.shape[0]
    mode_count = lon_count // 2
    wavenum = lax.broadcasted_iota(jnp.int32, (mode_count, lon_count), 0)
    longitude = lax.broadcasted_iota(jnp.int32, (mode_count, lon_count), 1)
    angles = phase_angle(wavenum, longitude, lon_count)
    real_part = jnp.dot(
        jnp.cos(angles) * factor,
        gathered,
        precision=lax.Precision.HIGHEST,
        preferred_element_type=jnp.float32,
    )
    imag_part = jnp.dot(
        -jnp.sin(angles) * factor,
        gathered,
        precision=lax.Precision.HIGHEST,
        preferred_element_type=jnp.float32,
    )
    return jnp.stack([real_part, imag_part])


def dense_local(state):
    lon_dev, fields, lat_dev = state.shape
    devices = lax.axis_size("lon")
    columns = state.reshape(lon_dev, fields * lat_dev)
    factor = 1.0 / math.sqrt(lon_dev * devices)
    gathered = lax.all_to_all(columns, "lon", split_axis=1, concat_axis=0, tiled=True)
    spectrum = dense_spectrum(gathered, factor)
    shares = lax.all_to_all(spectrum, "lon", split_axis=1, concat_axis=2, tiled=True)
    return shares.reshape(2, shares.shape[1], fields, lat_dev)


def split(value):
    high = value.astype(jnp.bfloat16)
    return high, (value - high.astype(jnp.float32)).astype(jnp.bfloat16)


def build_weights(cos_base, sin_base, cos_turn, sin_turn, w_hi, w_lo):
    modes, points = cos_base.shape

    def put(group, row, column, value):
        high, low = split(value)
        rows, columns = pl.ds(row * modes, modes), pl.ds(column * points, points)
        w_hi[group, rows, columns] = high
        w_lo[group, rows, columns] = low

    def table(residue):
        turn_c = cos_turn[pl.ds(residue, 1), :]
        turn_s = sin_turn[pl.ds(residue, 1), :]
        cos_b, sin_b = cos_base[...], sin_base[...]
        return cos_b * turn_c - sin_b * turn_s, sin_b * turn_c + cos_b * turn_s

    zero = jnp.zeros((modes, points), jnp.float32)
    for group in range(RADIX // 2):
        cos_a, sin_a = table(group)
        if group == 0:
            cos_b, sin_b = table(RADIX // 2)
            entries = ((cos_a, zero), (-sin_a, zero), (zero, cos_b), (zero, -sin_b))
        else:
            cos_b, sin_b = table(RADIX - group)
            entries = ((cos_a, sin_a), (-sin_a, cos_a), (cos_b, -sin_b), (-sin_b, -cos_b))
        for row, pair in enumerate(entries):
            for column, value in enumerate(pair):
                put(group, row, column, value)


def radix_stage(x):
    root = math.sqrt(0.5)
    a, b, c, d = x[0] + x[4], x[0] - x[4], x[2] + x[6], x[2] - x[6]
    e, f, g, h = x[1] + x[5], x[1] - x[5], x[3] + x[7], x[3] - x[7]
    even, odd = a + c, e + g
    diff, total = root * (f - h), root * (f + h)
    return (
        (even + odd, even - odd),
        (b + diff, -d - total),
        (a - c, g - e),
        (b - diff, d - total),
    )


def transform(half, points, grid, packed, w_hi, w_lo, y_hi, y_lo):
    modes = points // 2
    share = modes // RADIX
    block_rows = share * RADIX
    grid_rows = grid.reshape(grid.shape[0] * RADIX * points * SUBLANES, LANES)
    packed_rows = packed.reshape(packed.shape[0] * RADIX * 2 * block_rows * SUBLANES, LANES)

    def field_pair(pair, carry):
        def tile(index, carry):
            first = index * TILE
            for side in range(2):
                x = [
                    grid_rows[
                        pl.ds(
                            ((half * RADIX + d) * points + first) * SUBLANES + 2 * pair + side,
                            TILE,
                            stride=SUBLANES,
                        ),
                        :,
                    ]
                    for d in range(RADIX)
                ]
                for group, values in enumerate(radix_stage(x)):
                    for part, value in enumerate(values):
                        high, low = split(value)
                        rows = pl.ds(pl.multiple_of(part * points + first, TILE), TILE)
                        lanes = pl.ds(side * LANES, LANES)
                        y_hi[group, rows, lanes] = high
                        y_lo[group, rows, lanes] = low
            return carry

        lax.fori_loop(0, points // TILE, tile, 0)

        def residues(group, carry):
            dot = functools.partial(jnp.dot, preferred_element_type=jnp.float32)
            high = y_hi[group]
            out = dot(w_hi[group], high) + dot(w_hi[group], y_lo[group]) + dot(w_lo[group], high)
            other = jnp.where(group == 0, RADIX // 2, RADIX - group)
            for which, residue in enumerate((group, other)):
                for part in range(2):
                    row = (2 * which + part) * modes
                    for e in range(RADIX):
                        for side in range(2):
                            base = ((half * RADIX + e) * 2 + part) * block_rows
                            packed_rows[
                                pl.ds(
                                    (base + residue) * SUBLANES + 2 * pair + side,
                                    share,
                                    stride=RADIX * SUBLANES,
                                ),
                                :,
                            ] = out[
                                row + e * share : row + (e + 1) * share,
                                side * LANES : (side + 1) * LANES,
                            ]
            return carry

        lax.fori_loop(0, RADIX // 2, residues, 0)
        return carry

    lax.fori_loop(0, SUBLANES // 2, field_pair, 0)


def kernel(
    halves,
    state, cos_base, sin_base, cos_turn, sin_turn, out,
    grid, packed, w_hi, w_lo, y_hi, y_lo,
    send_sem, recv_sem, own_sem,
):
    points = state.shape[0]
    me = lax.axis_index("lon")
    ring, side = me // 2, lax.rem(me, 2)

    def peer(dz, dx):
        return lax.rem(ring + dz + 4, 4) * 2 + lax.rem(side + dx, 2)

    offsets = [(2, 1), (2, 0), (1, 1), (1, 0), (3, 1), (3, 0), (0, 1)]

    def fields(owner):
        return pl.ds(pl.multiple_of(owner * SUBLANES, SUBLANES), SUBLANES)

    def lanes(half):
        return pl.ds(half * LANES, LANES)

    def source(phase, half, target):
        if phase == 0:
            return state.at[:, fields(target), lanes(half)]
        return packed.at[half, target]

    def landing(phase, half, origin):
        if phase == 0:
            return grid.at[half, origin]
        return out.at[:, :, fields(origin), lanes(half)]

    def direct(phase, half, index):
        target = peer(*offsets[index])
        return pltpu.make_async_remote_copy(
            src_ref=source(phase, half, target),
            dst_ref=landing(phase, half, me),
            send_sem=send_sem.at[phase, half, index],
            recv_sem=recv_sem.at[phase, half, index],
            device_id={"lon": target},
            device_id_type=pl.DeviceIdType.MESH,
        )

    def own(phase, half):
        return pltpu.make_async_copy(
            source(phase, half, me), landing(phase, half, me), own_sem.at[phase, half]
        )

    def send(phase, half):
        for index in range(len(offsets)):
            direct(phase, half, index).start()
        own(phase, half).start()

    def receive(phase, half):
        own(phase, half).wait()
        for index, (dz, dx) in enumerate(offsets):
            origin = peer(-dz, dx)
            pltpu.make_async_remote_copy(
                src_ref=landing(phase, half, origin),
                dst_ref=landing(phase, half, origin),
                send_sem=send_sem.at[phase, half, index],
                recv_sem=recv_sem.at[phase, half, index],
                device_id={"lon": origin},
                device_id_type=pl.DeviceIdType.MESH,
            ).wait_recv()

    barrier = pltpu.get_barrier_semaphore()
    for dz, dx in offsets:
        pl.semaphore_signal(
            barrier, inc=1, device_id={"lon": peer(dz, dx)}, device_id_type=pl.DeviceIdType.MESH
        )
    pl.semaphore_wait(barrier, len(offsets))

    for half in range(halves):
        send(0, half)
    build_weights(cos_base, sin_base, cos_turn, sin_turn, w_hi, w_lo)
    for half in range(halves):
        receive(0, half)
        transform(half, points, grid, packed, w_hi, w_lo, y_hi, y_lo)
        send(1, half)
    for half in range(halves):
        receive(1, half)
    for phase in range(2):
        for half in range(halves):
            for index in range(len(offsets)):
                direct(phase, half, index).wait_send()


def angle_tables(points):
    count = points * RADIX
    scale = 1.0 / math.sqrt(count)
    place = np.arange(points)
    base = 2.0 * np.pi / count * (RADIX * np.arange(points // 2)[:, None] * place % count)
    turn = 2.0 * np.pi / count * (np.arange(RADIX)[:, None] * place % count)
    tables = (scale * np.cos(base), scale * np.sin(base), np.cos(turn), np.sin(turn))
    return [jnp.asarray(table.astype(np.float32)) for table in tables]


def fused_local(state):
    points, fields, lat_dev = state.shape
    halves = lat_dev // LANES
    modes = points // 2
    vmem = pl.BlockSpec(memory_space=pltpu.VMEM)
    hbm = pl.BlockSpec(memory_space=pl.ANY)
    half_shape = (2, modes, SUBLANES, LANES)
    return pl.pallas_call(
        functools.partial(kernel, halves),
        out_shape=jax.ShapeDtypeStruct((2, modes, fields, lat_dev), jnp.float32),
        in_specs=[hbm] + [vmem] * 4,
        out_specs=hbm,
        scratch_shapes=[
            pltpu.VMEM((halves, RADIX, points, SUBLANES, LANES), jnp.float32),
            pltpu.VMEM((halves, RADIX) + half_shape, jnp.float32),
            pltpu.VMEM((RADIX // 2, 4 * modes, 2 * points), jnp.bfloat16),
            pltpu.VMEM((RADIX // 2, 4 * modes, 2 * points), jnp.bfloat16),
            pltpu.VMEM((RADIX // 2, 2 * points, 2 * LANES), jnp.bfloat16),
            pltpu.VMEM((RADIX // 2, 2 * points, 2 * LANES), jnp.bfloat16),
            pltpu.SemaphoreType.DMA((2, halves, RADIX - 1)),
            pltpu.SemaphoreType.DMA((2, halves, RADIX - 1)),
            pltpu.SemaphoreType.DMA((2, halves)),
        ],
        compiler_params=pltpu.CompilerParams(
            collective_id=0, has_side_effects=True, vmem_limit_bytes=60 * 1024 * 1024
        ),
    )(state, *angle_tables(points))


def solution(mesh):
    devices = mesh.shape["lon"]

    def local(state):
        points, fields, lat_dev = state.shape
        fits = (
            devices == RADIX
            and fields == RADIX * SUBLANES
            and points == 2 * LANES
            and lat_dev == 2 * LANES
        )
        return fused_local(state) if fits else dense_local(state)

    return jax.shard_map(
        local,
        mesh=mesh,
        in_specs=(P("lon", None, "lat"),),
        out_specs=P(None, "lon", None, "lat"),
        check_vma=False,
    )
```

```python
import functools
import math

import jax
import jax.numpy as jnp
import numpy as np
from jax import lax
from jax.experimental import pallas as pl
from jax.experimental.pallas import tpu as pltpu
from jax.sharding import PartitionSpec as P

RADIX = 8
LANES = 128
SUBLANES = 8
TILE = 16


def phase_angle(first_index, second_index, period):
    product = first_index * second_index % period
    return product.astype(jnp.float32) * (2.0 * math.pi / period)


def dense_spectrum(gathered, factor):
    lon_count = gathered.shape[0]
    mode_count = lon_count // 2
    wavenum = lax.broadcasted_iota(jnp.int32, (mode_count, lon_count), 0)
    longitude = lax.broadcasted_iota(jnp.int32, (mode_count, lon_count), 1)
    angles = phase_angle(wavenum, longitude, lon_count)
    real_part = jnp.dot(
        jnp.cos(angles) * factor,
        gathered,
        precision=lax.Precision.HIGHEST,
        preferred_element_type=jnp.float32,
    )
    imag_part = jnp.dot(
        -jnp.sin(angles) * factor,
        gathered,
        precision=lax.Precision.HIGHEST,
        preferred_element_type=jnp.float32,
    )
    return jnp.stack([real_part, imag_part])


def dense_local(state):
    lon_dev, fields, lat_dev = state.shape
    devices = lax.axis_size("lon")
    columns = state.reshape(lon_dev, fields * lat_dev)
    factor = 1.0 / math.sqrt(lon_dev * devices)
    gathered = lax.all_to_all(columns, "lon", split_axis=1, concat_axis=0, tiled=True)
    spectrum = dense_spectrum(gathered, factor)
    shares = lax.all_to_all(spectrum, "lon", split_axis=1, concat_axis=2, tiled=True)
    return shares.reshape(2, shares.shape[1], fields, lat_dev)


def split(value):
    high = value.astype(jnp.bfloat16)
    return high, (value - high.astype(jnp.float32)).astype(jnp.bfloat16)


def build_weights(cos_base, sin_base, cos_turn, sin_turn, w_hi, w_lo):
    modes, points = cos_base.shape

    def put(group, row, column, value):
        high, low = split(value)
        rows, columns = pl.ds(row * modes, modes), pl.ds(column * points, points)
        w_hi[group, rows, columns] = high
        w_lo[group, rows, columns] = low

    def table(residue):
        turn_c = cos_turn[pl.ds(residue, 1), :]
        turn_s = sin_turn[pl.ds(residue, 1), :]
        cos_b, sin_b = cos_base[...], sin_base[...]
        return cos_b * turn_c - sin_b * turn_s, sin_b * turn_c + cos_b * turn_s

    zero = jnp.zeros((modes, points), jnp.float32)
    for group in range(RADIX // 2):
        cos_a, sin_a = table(group)
        if group == 0:
            cos_b, sin_b = table(RADIX // 2)
            entries = ((cos_a, zero), (-sin_a, zero), (zero, cos_b), (zero, -sin_b))
        else:
            cos_b, sin_b = table(RADIX - group)
            entries = ((cos_a, sin_a), (-sin_a, cos_a), (cos_b, -sin_b), (-sin_b, -cos_b))
        for row, pair in enumerate(entries):
            for column, value in enumerate(pair):
                put(group, row, column, value)


def radix_stage(x):
    root = math.sqrt(0.5)
    a, b, c, d = x[0] + x[4], x[0] - x[4], x[2] + x[6], x[2] - x[6]
    e, f, g, h = x[1] + x[5], x[1] - x[5], x[3] + x[7], x[3] - x[7]
    even, odd = a + c, e + g
    diff, total = root * (f - h), root * (f + h)
    return (
        (even + odd, even - odd),
        (b + diff, -d - total),
        (a - c, g - e),
        (b - diff, d - total),
    )


def transform(half, points, grid, packed, w_hi, w_lo, y_hi, y_lo):
    modes = points // 2
    share = modes // RADIX
    block_rows = share * RADIX
    grid_rows = grid.reshape(grid.shape[0] * RADIX * points * SUBLANES, LANES)
    packed_rows = packed.reshape(packed.shape[0] * RADIX * 2 * block_rows * SUBLANES, LANES)

    def field_pair(pair, carry):
        def tile(index, carry):
            first = index * TILE
            for side in range(2):
                x = [
                    grid_rows[
                        pl.ds(
                            ((half * RADIX + d) * points + first) * SUBLANES + 2 * pair + side,
                            TILE,
                            stride=SUBLANES,
                        ),
                        :,
                    ]
                    for d in range(RADIX)
                ]
                for group, values in enumerate(radix_stage(x)):
                    for part, value in enumerate(values):
                        high, low = split(value)
                        rows = pl.ds(pl.multiple_of(part * points + first, TILE), TILE)
                        lanes = pl.ds(side * LANES, LANES)
                        y_hi[group, rows, lanes] = high
                        y_lo[group, rows, lanes] = low
            return carry

        lax.fori_loop(0, points // TILE, tile, 0)

        def residues(group, carry):
            dot = functools.partial(jnp.dot, preferred_element_type=jnp.float32)
            high = y_hi[group]
            out = dot(w_hi[group], high) + dot(w_hi[group], y_lo[group]) + dot(w_lo[group], high)
            other = jnp.where(group == 0, RADIX // 2, RADIX - group)
            for which, residue in enumerate((group, other)):
                for part in range(2):
                    row = (2 * which + part) * modes
                    for e in range(RADIX):
                        for side in range(2):
                            base = ((half * RADIX + e) * 2 + part) * block_rows
                            packed_rows[
                                pl.ds(
                                    (base + residue) * SUBLANES + 2 * pair + side,
                                    share,
                                    stride=RADIX * SUBLANES,
                                ),
                                :,
                            ] = out[
                                row + e * share : row + (e + 1) * share,
                                side * LANES : (side + 1) * LANES,
                            ]
            return carry

        lax.fori_loop(0, RADIX // 2, residues, 0)
        return carry

    lax.fori_loop(0, SUBLANES // 2, field_pair, 0)


def kernel(
    halves,
    state, cos_base, sin_base, cos_turn, sin_turn, out,
    grid, packed, w_hi, w_lo, y_hi, y_lo,
    send_sem, recv_sem, own_sem,
):
    points = state.shape[0]
    me = lax.axis_index("lon")
    ring, side = me // 2, lax.rem(me, 2)

    def peer(dz, dx):
        return lax.rem(ring + dz + 4, 4) * 2 + lax.rem(side + dx, 2)

    offsets = [(2, 1), (2, 0), (1, 1), (1, 0), (3, 1), (3, 0), (0, 1)]

    def fields(owner):
        return pl.ds(pl.multiple_of(owner * SUBLANES, SUBLANES), SUBLANES)

    def lanes(half):
        return pl.ds(half * LANES, LANES)

    def source(phase, half, target):
        if phase == 0:
            return state.at[:, fields(target), lanes(half)]
        return packed.at[half, target]

    def landing(phase, half, origin):
        if phase == 0:
            return grid.at[half, origin]
        return out.at[:, :, fields(origin), lanes(half)]

    def direct(phase, half, index):
        target = peer(*offsets[index])
        return pltpu.make_async_remote_copy(
            src_ref=source(phase, half, target),
            dst_ref=landing(phase, half, me),
            send_sem=send_sem.at[phase, half, index],
            recv_sem=recv_sem.at[phase, half, index],
            device_id={"lon": target},
            device_id_type=pl.DeviceIdType.MESH,
        )

    def own(phase, half):
        return pltpu.make_async_copy(
            source(phase, half, me), landing(phase, half, me), own_sem.at[phase, half]
        )

    def send(phase, half):
        for index in range(len(offsets)):
            direct(phase, half, index).start()
        own(phase, half).start()

    def receive(phase, half):
        own(phase, half).wait()
        for index, (dz, dx) in enumerate(offsets):
            origin = peer(-dz, dx)
            pltpu.make_async_remote_copy(
                src_ref=landing(phase, half, origin),
                dst_ref=landing(phase, half, origin),
                send_sem=send_sem.at[phase, half, index],
                recv_sem=recv_sem.at[phase, half, index],
                device_id={"lon": origin},
                device_id_type=pl.DeviceIdType.MESH,
            ).wait_recv()

    barrier = pltpu.get_barrier_semaphore()
    for dz, dx in offsets:
        pl.semaphore_signal(
            barrier, inc=1, device_id={"lon": peer(dz, dx)}, device_id_type=pl.DeviceIdType.MESH
        )
    pl.semaphore_wait(barrier, len(offsets))

    for half in range(halves):
        send(0, half)
    build_weights(cos_base, sin_base, cos_turn, sin_turn, w_hi, w_lo)
    for half in range(halves):
        receive(0, half)
        transform(half, points, grid, packed, w_hi, w_lo, y_hi, y_lo)
        send(1, half)
    for half in range(halves):
        receive(1, half)
    for phase in range(2):
        for half in range(halves):
            for index in range(len(offsets)):
                direct(phase, half, index).wait_send()


def angle_tables(points):
    count = points * RADIX
    scale = 1.0 / math.sqrt(count)
    place = np.arange(points)
    base = 2.0 * np.pi / count * (RADIX * np.arange(points // 2)[:, None] * place % count)
    turn = 2.0 * np.pi / count * (np.arange(RADIX)[:, None] * place % count)
    tables = (scale * np.cos(base), scale * np.sin(base), np.cos(turn), np.sin(turn))
    return [jnp.asarray(table.astype(np.float32)) for table in tables]


def fused_local(state):
    points, fields, lat_dev = state.shape
    halves = lat_dev // LANES
    modes = points // 2
    vmem = pl.BlockSpec(memory_space=pltpu.VMEM)
    hbm = pl.BlockSpec(memory_space=pl.ANY)
    half_shape = (2, modes, SUBLANES, LANES)
    return pl.pallas_call(
        functools.partial(kernel, halves),
        out_shape=pltpu.VMEM((2, modes, fields, lat_dev), jnp.float32),
        in_specs=[hbm] + [vmem] * 4,
        out_specs=hbm,
        scratch_shapes=[
            pltpu.VMEM((halves, RADIX, points, SUBLANES, LANES), jnp.float32),
            pltpu.VMEM((halves, RADIX) + half_shape, jnp.float32),
            pltpu.VMEM((RADIX // 2, 4 * modes, 2 * points), jnp.bfloat16),
            pltpu.VMEM((RADIX // 2, 4 * modes, 2 * points), jnp.bfloat16),
            pltpu.VMEM((RADIX // 2, 2 * points, 2 * LANES), jnp.bfloat16),
            pltpu.VMEM((RADIX // 2, 2 * points, 2 * LANES), jnp.bfloat16),
            pltpu.SemaphoreType.DMA((2, halves, RADIX - 1)),
            pltpu.SemaphoreType.DMA((2, halves, RADIX - 1)),
            pltpu.SemaphoreType.DMA((2, halves)),
        ],
        compiler_params=pltpu.CompilerParams(
            collective_id=0, has_side_effects=True, vmem_limit_bytes=41 * 1024 * 1024
        ),
    )(state, *angle_tables(points))


def solution(mesh):
    devices = mesh.shape["lon"]

    def local(state):
        points, fields, lat_dev = state.shape
        fits = (
            devices == RADIX
            and fields == RADIX * SUBLANES
            and points == 2 * LANES
            and lat_dev == 2 * LANES
        )
        return fused_local(state) if fits else dense_local(state)

    return jax.shard_map(
        local,
        mesh=mesh,
        in_specs=(P("lon", None, "lat"),),
        out_specs=P(None, "lon", None, "lat"),
        check_vma=False,
    )
```
